512 devices in a mesh: row: 8 (over y), col: 32 (over z, x), layer: 2 (over core).
Axes of the slice: x: 4, y: 8, z: 8, core: 2. Of those that a mesh axis runs over, the one named last changes fastest.
Arguments:
- anomaly_x: bfloat16 [8, 4096, 4096], P(None, 'row', ('layer', 'col')), may hold values from -0.09375 to 0.09375
- anomaly_y: bfloat16 [8, 4096, 4096], P(None, 'col', ('layer', 'row')), may hold values from -6 to 6
Outputs:
- covariance: bfloat16 [8, 4096, 4096], P('layer', 'row', 'col')
The draws below stay inside these ranges and needn't reach their ends.
All inputs are finite; a program needn't handle non-finite values.
Results may differ from the reference program's by a relative error of at most 0.001.
Values may be sent and summed in bfloat16 or wider, within the bound.
A program may use at most 64 MiB of HBM per device.

```python
import jax
import jax.numpy as jnp
from jax import lax

BATCH = 8
NSTATE = 4096
MEMBERS = 4096


def raised(values, own_key, source, target, shards_of, factor):
    owner, partner = [(jnp.arange(values.shape[axis_at]) // (values.shape[axis_at] // shards_of)).reshape([-1 if axis == axis_at else 1 for axis in range(values.ndim)]) for axis_at in (source, target)]
    chosen = jax.random.permutation(own_key, shards_of)[partner]
    strong = (owner == chosen) | (owner == (partner + shards_of // 2) % shards_of)
    return jnp.where(strong, factor * values, values)


def steps_of(rng, dims, cuts, least, top_value):
    level, own = 1.0, jax.random.fold_in(rng, 6)
    for position, shards_of in cuts:
        steps = jnp.exp(jax.random.uniform(jax.random.fold_in(own, position), (shards_of,), jnp.float32, least / len(cuts), top_value / len(cuts)))
        level = level * jnp.repeat(steps, dims[position] // shards_of).reshape([-1 if axis == position else 1 for axis in range(len(dims))])
    return level


def noise(rng, shape, deviation, reach, pieces=(), held_as=jnp.bfloat16):
    gain = steps_of(rng, shape, pieces, -0.22, 0.18) if pieces else 1.0
    drawn = jax.random.normal(rng, shape, jnp.float32) * deviation * gain
    return jnp.minimum(jnp.maximum(drawn, -reach), reach).astype(held_as)


def heavy_noise(stream_key, dims, deviation, reach, shards, heavy, kind=jnp.bfloat16):
    result = deviation * jax.random.normal(stream_key, dims, jnp.float32)
    if shards:
        result = result * steps_of(stream_key, dims, shards, -0.22, 0.18)
    return jnp.clip(raised(result, jax.random.fold_in(stream_key, 3), *heavy), -reach, reach).astype(kind)


def setup_inputs(seed: int = 0) -> dict:
    key_of = jax.random.split(jax.random.key(seed), 3)
    return {
        "anomaly_x": noise(key_of[0], (BATCH, NSTATE, MEMBERS), MEMBERS ** -0.5, 0.09375, ((1, 8), (2, 64))),
        "anomaly_y": heavy_noise(key_of[1], (BATCH, NSTATE, MEMBERS), 1.0, 6.0, ((1, 32), (2, 16)), (2, 0, 8, 2.0)),
    }


def one_product(pair):
    left, right = pair
    return jnp.dot(left, right.T, preferred_element_type=jnp.float32).astype(jnp.bfloat16)


def reference(anomaly_x, anomaly_y):
    return lax.map(one_product, (anomaly_x, anomaly_y))
```

```python
import jax
import jax.numpy as jnp
from jax import lax
from jax.experimental import pallas as pl
from jax.experimental.pallas import tpu as pltpu
from jax.sharding import PartitionSpec as P

MESH = pl.DeviceIdType.MESH
RING = 8
LINE = 4
OFFSETS = (0, 1, 3, 2)
BACK = (0, 2, 1, 3)


def kernel(
    x_hbm, y_hbm, out_ref, x_in, y_in, xg, yg, acc, tile, in_sem, own_sem,
    a_send, a_recv, g_send, g_recv, c_send, c_recv,
):
    row, col, layer = lax.axis_index("row"), lax.axis_index("col"), lax.axis_index("layer")
    z, x = col // LINE, lax.rem(col, LINE)
    mine = layer * LINE + x

    def at(row_to, z_to, x_to, layer_to):
        return {"row": row_to, "col": z_to * LINE + x_to, "layer": layer_to}

    def step_x(p):
        return lax.rem(x + OFFSETS[p], LINE)

    def along(pos, by):
        return lax.rem(pos + by + RING, RING)

    pos = (z, row)
    inputs = (x_in, y_in)
    gathered = (xg, yg)
    depth = (64, 128)

    def place(kind, chunk, part, x_from):
        span = pl.ds(pl.multiple_of(x_from * depth[kind], depth[kind]), depth[kind])
        return gathered[kind].at[chunk, part, span, :]

    def neighbour(kind, by):
        if kind == 0:
            return at(row, along(z, by), x, layer)
        return at(along(row, by), z, x, layer)

    loads = [
        pltpu.make_async_copy(x_hbm, x_in, in_sem.at[0]),
        pltpu.make_async_copy(y_hbm, y_in, in_sem.at[1]),
    ]
    own = [
        pltpu.make_async_copy(x_hbm.at[mine], place(0, z, layer, x), own_sem.at[0]),
        pltpu.make_async_copy(y_hbm.at[mine], place(1, row, layer, x), own_sem.at[1]),
    ]
    for copy in loads + own:
        copy.start()

    barrier = pltpu.get_barrier_semaphore()
    other = 1 - layer
    peers = [at(row, z, x, other)]
    peers += [at(row, z, step_x(p), to) for p in (1, 2, 3) for to in (0, 1)]
    peers += [neighbour(kind, by) for kind in (0, 1) for by in (1, -1)]
    for peer in peers:
        pl.semaphore_signal(barrier, inc=1, device_id=peer, device_id_type=MESH)
    acc[...] = jnp.zeros_like(acc)
    pl.semaphore_wait(barrier, len(peers))
    for copy in loads:
        copy.wait()

    def deal(kind, p, to):
        x_to = step_x(p)
        return pltpu.make_async_remote_copy(
            src_ref=inputs[kind].at[to * LINE + x_to],
            dst_ref=place(kind, pos[kind], layer, x),
            send_sem=a_send.at[kind, p, to],
            recv_sem=a_recv.at[kind, BACK[p], layer],
            device_id=at(row, z, x_to, to),
            device_id_type=MESH,
        )

    def dealt(kind, p, origin):
        block = place(kind, pos[kind], origin, step_x(p))
        return pltpu.make_async_remote_copy(
            src_ref=block,
            dst_ref=block,
            send_sem=a_send.at[kind, p, origin],
            recv_sem=a_recv.at[kind, p, origin],
            device_id=at(row, z, x, other),
            device_id_type=MESH,
        )

    deals = [deal(kind, 0, other) for kind in (0, 1)]
    deals += [deal(kind, p, to) for p in (1, 2, 3) for kind in (0, 1) for to in (0, 1)]
    for copy in deals:
        copy.start()

    def piece(kind, chunk, p):
        return place(kind, chunk, slice(None), step_x(p))

    def forward(kind, way, step, p):
        by = 1 if way == 0 else -1
        chunk = along(pos[kind], -by * step)
        block = piece(kind, chunk, p)
        return pltpu.make_async_remote_copy(
            src_ref=block,
            dst_ref=block,
            send_sem=g_send.at[kind, way, step, p],
            recv_sem=g_recv.at[kind, chunk, p],
            device_id=neighbour(kind, by),
            device_id_type=MESH,
        )

    def arrived(kind, way, step, p):
        by = 1 if way == 0 else -1
        chunk = along(pos[kind], -by * step)
        block = piece(kind, chunk, p)
        return pltpu.make_async_remote_copy(
            src_ref=block,
            dst_ref=block,
            send_sem=g_send.at[kind, way, 0, p],
            recv_sem=g_recv.at[kind, chunk, p],
            device_id=neighbour(kind, by),
            device_id_type=MESH,
        )

    def apart(a, b):
        return jnp.minimum(lax.rem(a - b + RING, RING), lax.rem(b - a + RING, RING))

    def multiply(step):
        def body(chunk, carry):
            @pl.when(jnp.maximum(apart(chunk, z), apart(chunk, row)) == step)
            def _():
                total = acc[...]
                for part in (0, 1):
                    total += jnp.dot(yg[chunk, part], xg[chunk, part], preferred_element_type=jnp.float32)
                acc[...] = total

            return carry

        lax.fori_loop(0, RING, body, 0)

    forwards = []
    for step in range(5):
        for p in range(LINE):
            for kind in (0, 1):
                if step == 0:
                    if p == 0:
                        own[kind].wait()
                        dealt(kind, 0, other).wait_recv()
                    else:
                        dealt(kind, p, 0).wait_recv()
                        dealt(kind, p, 1).wait_recv()
                for way in (0, 1):
                    odd = p % 2 == way
                    if step == 4 and not odd:
                        continue
                    if step > 0:
                        arrived(kind, way, step, p).wait_recv()
                    if step < 3 or (step == 3 and odd):
                        copy = forward(kind, way, step, p)
                        copy.start()
                        forwards.append(copy)
        multiply(step)

    def hand(p):
        x_to = step_x(p)
        return pltpu.make_async_remote_copy(
            src_ref=tile.at[p],
            dst_ref=out_ref.at[x],
            send_sem=c_send.at[p],
            recv_sem=c_recv.at[BACK[p]],
            device_id=at(row, z, x_to, layer),
            device_id_type=MESH,
        )

    def handed(p):
        block = out_ref.at[step_x(p)]
        return pltpu.make_async_remote_copy(
            src_ref=block,
            dst_ref=block,
            send_sem=c_send.at[p],
            recv_sem=c_recv.at[p],
            device_id=at(row, z, step_x(p), layer),
            device_id_type=MESH,
        )

    hands = []
    for p in (3, 1, 2, 0):
        x_to = step_x(p)
        rows = acc[pl.ds(pl.multiple_of(x_to * 128, 128), 128), :]
        block = rows.T.astype(jnp.bfloat16)
        if p == 0:
            out_ref[x] = block
        else:
            tile[p] = block
            copy = hand(p)
            copy.start()
            hands.append(copy)
    for copy in deals + forwards + hands:
        copy.wait_send()
    for p in (1, 2, 3):
        handed(p).wait_recv()


def on_device(anomaly_x, anomaly_y):
    dma = pltpu.SemaphoreType.DMA
    return pl.pallas_call(
        kernel,
        out_shape=jax.ShapeDtypeStruct((4, 512, 128), jnp.bfloat16),
        in_specs=[pl.BlockSpec(memory_space=pl.ANY)] * 2,
        out_specs=pl.BlockSpec(memory_space=pltpu.VMEM),
        scratch_shapes=[
            pltpu.VMEM((8, 64, 512), jnp.bfloat16),
            pltpu.VMEM((8, 128, 256), jnp.bfloat16),
            pltpu.VMEM((RING, 2, 256, 512), jnp.bfloat16),
            pltpu.VMEM((RING, 2, 512, 256), jnp.bfloat16),
            pltpu.VMEM((512, 512), jnp.float32),
            pltpu.VMEM((LINE, 512, 128), jnp.bfloat16),
            dma((2,)),
            dma((2,)),
            dma((2, LINE, 2)),
            dma((2, LINE, 2)),
            dma((2, 2, 4, LINE)),
            dma((2, RING, LINE)),
            dma((LINE,)),
            dma((LINE,)),
        ],
        compiler_params=pltpu.CompilerParams(collective_id=0, has_side_effects=True),
    )(jnp.transpose(anomaly_x, (0, 2, 1)), anomaly_y)


def solution(mesh):
    placed = (P(None, "row", ("layer", "col")), P(None, "col", ("layer", "row")))
    return jax.shard_map(
        on_device, mesh=mesh, in_specs=placed, out_specs=P("layer", "row", "col"), check_vma=False
    )
```

```python
import jax
import jax.numpy as jnp
from jax import lax
from jax.experimental import pallas as pl
from jax.experimental.pallas import tpu as pltpu
from jax.sharding import PartitionSpec as P

MESH = pl.DeviceIdType.MESH
RING = 8
LINE = 4
OFFSETS = (0, 1, 3, 2)
BACK = (0, 2, 1, 3)
ORDERS = (
    (
        ((0, 0), (0, 1), (0, 2), (1, 0), (0, 3), (2, 0), (1, 3), (1, 1), (3, 0), (2, 3), (1, 2), (2, 1), (3, 3), (2, 2)),
        ((0, 0), (0, 1), (0, 2), (1, 1), (1, 2), (0, 3), (2, 1), (2, 2), (1, 0), (3, 1), (1, 3), (2, 0), (3, 2), (2, 3)),
    ),
    (
        ((0, 0), (1, 0), (0, 1), (0, 2), (1, 1), (0, 3), (1, 2), (1, 3), (2, 2), (2, 3), (2, 0), (3, 3), (2, 1), (3, 0)),
        ((0, 0), (1, 0), (0, 1), (0, 2), (1, 1), (0, 3), (1, 2), (1, 3), (2, 2), (2, 1), (3, 2), (2, 3), (3, 1), (2, 0)),
    ),
)


def kernel(
    x_hbm, y_hbm, out_ref, x_in, y_in, xg, yg, acc, tile, in_sem, own_sem,
    a_send, a_recv, g_send, g_recv, l_send, l_recv, c_send, c_recv,
):
    row, col, layer = lax.axis_index("row"), lax.axis_index("col"), lax.axis_index("layer")
    z, x = col // LINE, lax.rem(col, LINE)
    mine = layer * LINE + x

    def at(row_to, z_to, x_to, layer_to):
        return {"row": row_to, "col": z_to * LINE + x_to, "layer": layer_to}

    def step_x(p):
        return lax.rem(x + OFFSETS[p], LINE)

    def along(pos, by):
        return lax.rem(pos + by + RING, RING)

    pos = (z, row)
    inputs = (x_in, y_in)
    gathered = (xg, yg)
    depth = (64, 128)

    def place(kind, chunk, part, x_from):
        span = pl.ds(pl.multiple_of(x_from * depth[kind], depth[kind]), depth[kind])
        return gathered[kind].at[chunk, part, span, :]

    def neighbour(kind, by):
        if kind == 0:
            return at(row, along(z, by), x, layer)
        return at(along(row, by), z, x, layer)

    loads = [
        pltpu.make_async_copy(x_hbm, x_in, in_sem.at[0]),
        pltpu.make_async_copy(y_hbm, y_in, in_sem.at[1]),
    ]
    own = [
        pltpu.make_async_copy(x_hbm.at[mine], place(0, z, layer, x), own_sem.at[0]),
        pltpu.make_async_copy(y_hbm.at[mine], place(1, row, layer, x), own_sem.at[1]),
    ]
    for copy in loads + own:
        copy.start()

    barrier = pltpu.get_barrier_semaphore()
    other = 1 - layer
    peers = [at(row, z, x, other)]
    peers += [at(row, z, step_x(p), to) for p in (1, 2, 3) for to in (0, 1)]
    peers += [neighbour(kind, by) for kind in (0, 1) for by in (1, -1)]
    for peer in peers:
        pl.semaphore_signal(barrier, inc=1, device_id=peer, device_id_type=MESH)
    pl.semaphore_wait(barrier, len(peers))
    for copy in loads:
        copy.wait()

    def deal(kind, p, to):
        x_to = step_x(p)
        return pltpu.make_async_remote_copy(
            src_ref=inputs[kind].at[to * LINE + x_to],
            dst_ref=place(kind, pos[kind], layer, x),
            send_sem=a_send.at[kind, p, to],
            recv_sem=a_recv.at[kind, BACK[p], layer],
            device_id=at(row, z, x_to, to),
            device_id_type=MESH,
        )

    def dealt(kind, p, origin):
        block = place(kind, pos[kind], origin, step_x(p))
        return pltpu.make_async_remote_copy(
            src_ref=block,
            dst_ref=block,
            send_sem=a_send.at[kind, p, origin],
            recv_sem=a_recv.at[kind, p, origin],
            device_id=at(row, z, x, other),
            device_id_type=MESH,
        )

    deals = [deal(kind, 0, other) for kind in (0, 1)]
    deals += [deal(kind, p, to) for kind in (0, 1) for p in (1, 2) for to in (0, 1)]
    deals += [deal(kind, 3, to) for kind in (0, 1) for to in (0, 1)]
    for copy in deals:
        copy.start()

    def piece(kind, chunk, p):
        return place(kind, chunk, slice(None), step_x(p))

    def forward(kind, way, step, p):
        by = 1 if way == 0 else -1
        chunk = along(pos[kind], -by * step)
        block = piece(kind, chunk, p)
        return pltpu.make_async_remote_copy(
            src_ref=block,
            dst_ref=block,
            send_sem=g_send.at[kind, way, step, p],
            recv_sem=g_recv.at[kind, chunk, p],
            device_id=neighbour(kind, by),
            device_id_type=MESH,
        )

    def arrived(kind, way, step, p):
        by = 1 if way == 0 else -1
        chunk = along(pos[kind], -by * step)
        block = piece(kind, chunk, p)
        return pltpu.make_async_remote_copy(
            src_ref=block,
            dst_ref=block,
            send_sem=g_send.at[kind, way, 0, p],
            recv_sem=g_recv.at[kind, chunk, p],
            device_id=neighbour(kind, by),
            device_id_type=MESH,
        )

    def quarter(q):
        return pl.ds(q * 128, 128)

    def last(way, step, p, q):
        by = 1 if way == 0 else -1
        block = piece(0, along(z, -by * step), p).at[:, :, quarter(q)]
        sem = (way, step - 2, q)
        return pltpu.make_async_remote_copy(
            src_ref=block,
            dst_ref=block,
            send_sem=l_send.at[sem],
            recv_sem=l_recv.at[sem],
            device_id=neighbour(0, by),
            device_id_type=MESH,
        )

    def last_arrived(way, step, p, q):
        by = 1 if way == 0 else -1
        block = piece(0, along(z, -by * (step + 1)), p).at[:, :, quarter(q)]
        sem = (way, step - 2, q)
        return pltpu.make_async_remote_copy(
            src_ref=block,
            dst_ref=block,
            send_sem=l_send.at[sem],
            recv_sem=l_recv.at[sem],
            device_id=neighbour(0, by),
            device_id_type=MESH,
        )

    def rows_of(p):
        return pl.ds(pl.multiple_of(step_x(p) * 128, 128), 128)

    def product(p, nears, columns):
        total = None
        for near in nears:
            chunk = along(z, near)
            for part in (0, 1):
                term = jnp.dot(
                    yg[chunk, part, rows_of(p), :], xg[chunk, part, :, columns], preferred_element_type=jnp.float32
                )
                total = term if total is None else total + term
        return total

    sent = list(deals)
    have = [set(), set()]

    def take(kind, way, step, p):
        if step == 0:
            if p in have[kind]:
                return
            have[kind].add(p)
            if p == 0:
                own[kind].wait()
                dealt(kind, 0, other).wait_recv()
            else:
                dealt(kind, p, 0).wait_recv()
                dealt(kind, p, 1).wait_recv()
        else:
            arrived(kind, way, step, p).wait_recv()

    taken = set()

    def turn(kind, way, i):
        step, p = ORDERS[kind][way][i]
        take(kind, way, step, p)
        taken.add((kind, way, step, p))
        if kind == 0 and i >= 12:
            return
        copy = forward(kind, way, step, p)
        copy.start()
        sent.append(copy)

    for i in range(14):
        for kind in (0, 1):
            for way in (0, 1):
                turn(kind, way, i)
    for q in range(4):
        for i in (12, 13):
            for way in (0, 1):
                copy = last(way, *ORDERS[0][way][i], q)
                copy.start()
                sent.append(copy)
    lasts = [(way, *ORDERS[0][way][i]) for i in (12, 13) for way in (0, 1)]
    late = {(way, step + 1, p) for way, step, p in lasts}
    for kind in (0, 1):
        for way in (0, 1):
            for step, p in ORDERS[kind][way]:
                key = (kind, way, step + 1, p)
                if key in taken or (kind == 0 and key[1:] in late) or (kind == 1 and p < 2):
                    continue
                arrived(*key).wait_recv()
                taken.add(key)

    def rest(p):
        for way in (0, 1):
            for step, p_of in ORDERS[1][way]:
                key = (1, way, step + 1, p_of)
                if p_of == p and key not in taken:
                    arrived(*key).wait_recv()
                    taken.add(key)

    def hand(p, q):
        return pltpu.make_async_remote_copy(
            src_ref=tile.at[p, quarter(q)],
            dst_ref=out_ref.at[x, quarter(q)],
            send_sem=c_send.at[p, q],
            recv_sem=c_recv.at[BACK[p], q],
            device_id=at(row, z, step_x(p), layer),
            device_id_type=MESH,
        )

    def handed(p, q):
        block = out_ref.at[step_x(p), quarter(q)]
        return pltpu.make_async_remote_copy(
            src_ref=block,
            dst_ref=block,
            send_sem=c_send.at[p, q],
            recv_sem=c_recv.at[p, q],
            device_id=at(row, z, step_x(p), layer),
            device_id_type=MESH,
        )

    def early(p):
        acc[p] = product(p, (0, 1, -1, 2, -2), slice(None))

    def finish(p, q):
        block = (acc[p, :, quarter(q)] + product(p, (3, -3, 4), quarter(q))).T.astype(jnp.bfloat16)
        if p == 0:
            out_ref[x, quarter(q)] = block
        else:
            tile[p, quarter(q)] = block
            copy = hand(p, q)
            copy.start()
            sent.append(copy)

    early(3)
    early(2)
    for q in range(4):
        for key in lasts:
            last_arrived(*key, q).wait_recv()
        finish(3, q)
        finish(2, q)
        if q == 0:
            rest(1)
            early(1)
        finish(1, q)
    rest(0)
    early(0)
    for q in range(4):
        finish(0, q)
    for copy in sent:
        copy.wait_send()
    for p in (1, 2, 3):
        for q in range(4):
            handed(p, q).wait_recv()


def on_device(anomaly_x, anomaly_y):
    dma = pltpu.SemaphoreType.DMA
    return pl.pallas_call(
        kernel,
        out_shape=pltpu.VMEM((4, 512, 128), jnp.bfloat16),
        in_specs=[pl.BlockSpec(memory_space=pl.ANY)] * 2,
        out_specs=pl.BlockSpec(memory_space=pltpu.VMEM),
        scratch_shapes=[
            pltpu.VMEM((8, 64, 512), jnp.bfloat16),
            pltpu.VMEM((8, 128, 256), jnp.bfloat16),
            pltpu.VMEM((RING, 2, 256, 512), jnp.bfloat16),
            pltpu.VMEM((RING, 2, 512, 256), jnp.bfloat16),
            pltpu.VMEM((LINE, 128, 512), jnp.float32),
            pltpu.VMEM((LINE, 512, 128), jnp.bfloat16),
            dma((2,)),
            dma((2,)),
            dma((2, LINE, 2)),
            dma((2, LINE, 2)),
            dma((2, 2, 4, LINE)),
            dma((2, RING, LINE)),
            dma((2, 2, 4)),
            dma((2, 2, 4)),
            dma((LINE, 4)),
            dma((LINE, 4)),
        ],
        compiler_params=pltpu.CompilerParams(collective_id=0, has_side_effects=True),
    )(jnp.transpose(anomaly_x, (0, 2, 1)), anomaly_y)


def solution(mesh):
    placed = (P(None, "row", ("layer", "col")), P(None, "col", ("layer", "row")))
    return jax.shard_map(
        on_device, mesh=mesh, in_specs=placed, out_specs=P("layer", "row", "col"), check_vma=False
    )
```

```python
import jax
import jax.numpy as jnp
from jax import lax
from jax.experimental import pallas as pl
from jax.experimental.pallas import tpu as pltpu
from jax.sharding import PartitionSpec as P

MESH = pl.DeviceIdType.MESH
RING = 8
LINE = 4
OFFSETS = (0, 1, 3, 2)
BACK = (0, 2, 1, 3)
UNITS = {"a": ("a",), "b": ("b",), 0: ("a", "b"), 1: (1,), 2: (2,), 3: (3,), "A": ("a", "b", 3), "B": (1, 2)}
SLOT = {"a": 0, "b": 4, 0: 0, 1: 1, 2: 2, 3: 3, "A": 5, "B": 6}
TURNS = (
    (0, 0, 0, "a"), (0, 1, 0, "a"), (1, 0, 0, "a"), (1, 1, 0, "a"), (0, 0, 0, "b"), (0, 1, 0, "b"),
    (1, 0, 0, "b"), (1, 1, 0, "b"), (0, 0, 1, "a"), (0, 1, 1, "a"), (1, 0, 1, "a"), (1, 1, 1, "a"),
    (0, 0, 0, 1), (0, 1, 0, 1), (1, 0, 0, 2), (1, 1, 0, 2), (1, 0, 1, "b"), (0, 0, 0, 2),
    (0, 1, 0, 2), (1, 1, 0, 1), (1, 0, 0, 1), (0, 0, 1, "b"), (0, 1, 1, "b"), (1, 1, 1, 2),
    (1, 0, 1, 2), (0, 0, 0, 3), (0, 1, 0, 3), (0, 0, 1, "B"), (0, 1, 1, "B"), (1, 1, 0, 3),
    (1, 0, 0, 3), (1, 1, 1, 1), (1, 0, 2, 0), (1, 1, 1, "b"), (0, 0, 1, 3), (0, 1, 1, 3),
    (1, 1, 1, 3), (1, 0, 1, 3), (0, 0, 2, 0), (1, 0, 1, 1), (1, 1, 2, "B"), (0, 1, 2, "B"),
    (0, 0, 2, 3), (1, 0, 2, 3), (0, 1, 2, "A"), (0, 0, 2, "B"), (1, 1, 2, 3), (1, 0, 2, 2),
    (1, 1, 3, 2), (0, 1, 3, "B"), (1, 0, 3, 3), (0, 0, 3, "A"), (1, 1, 3, 1), (1, 0, 2, 1),
    (1, 1, 2, 0), (1, 0, 3, 0),)


def kernel(
    x_hbm, y_hbm, out_ref, x_in, y_in, xg, yg, acc, tile, in_sem, own_sem,
    a_send, a_recv, g_send, g_recv, l_send, l_recv, c_send, c_recv,
):
    row, col, layer = lax.axis_index("row"), lax.axis_index("col"), lax.axis_index("layer")
    z, x = col // LINE, lax.rem(col, LINE)
    other = 1 - layer
    mine = layer * LINE + x

    def at(row_to, z_to, x_to, layer_to):
        return {"row": row_to, "col": z_to * LINE + x_to, "layer": layer_to}

    def step_x(p):
        return lax.rem(x + OFFSETS[p], LINE)

    def along(pos, by):
        return lax.rem(pos + by + RING, RING)

    def send(src, dst, send_sem, recv_sem, device_id):
        return pltpu.make_async_remote_copy(
            src_ref=src, dst_ref=dst, send_sem=send_sem, recv_sem=recv_sem, device_id=device_id, device_id_type=MESH
        )

    pos = (z, row)
    inputs = (x_in, y_in)
    gathered = (xg, yg)

    def place(kind, chunk, part, x_from):
        return gathered[kind].at[chunk, part, x_from // 2, lax.rem(x_from, 2)]

    def pair(kind, chunk, which):
        parity = lax.rem(x + (0 if which == "A" else 1), 2)
        return gathered[kind].at[chunk, :, :, parity]

    def piece(kind, chunk, p):
        if p in ("A", "B"):
            return pair(kind, chunk, p)
        if p in ("a", "b"):
            return place(kind, chunk, layer if p == "a" else other, x)
        return place(kind, chunk, slice(None), step_x(p))

    def neighbour(kind, by):
        return at(row, along(z, by), x, layer) if kind == 0 else at(along(row, by), z, x, layer)

    loads = [
        pltpu.make_async_copy(x_hbm, x_in, in_sem.at[0]),
        pltpu.make_async_copy(y_hbm, y_in, in_sem.at[1]),
    ]
    own = [
        pltpu.make_async_copy(x_hbm.at[mine], place(0, z, layer, x), own_sem.at[0]),
        pltpu.make_async_copy(y_hbm.at[mine], place(1, row, layer, x), own_sem.at[1]),
    ]
    for copy in loads + own:
        copy.start()

    barrier = pltpu.get_barrier_semaphore()
    peers = [at(row, z, x, other)]
    peers += [at(row, z, step_x(p), to) for p in (1, 2, 3) for to in (0, 1)]
    peers += [neighbour(kind, by) for kind in (0, 1) for by in (1, -1)]
    for peer in peers:
        pl.semaphore_signal(barrier, inc=1, device_id=peer, device_id_type=MESH)
    pl.semaphore_wait(barrier, len(peers))
    for copy in loads:
        copy.wait()

    def deal(kind, p, to):
        x_to = step_x(p)
        return send(
            inputs[kind].at[to * LINE + x_to],
            place(kind, pos[kind], layer, x),
            a_send.at[kind, p, to],
            a_recv.at[kind, BACK[p], layer],
            at(row, z, x_to, to),
        )

    def dealt(kind, p, origin):
        block = place(kind, pos[kind], origin, step_x(p))
        return send(block, block, a_send.at[kind, p, origin], a_recv.at[kind, p, origin], at(row, z, x, other))

    deals = [deal(kind, 0, other) for kind in (0, 1)]
    for first, to in ((0, 0), (0, 1), (1, 0), (1, 1)):
        deals += [deal(first, 2, to), deal(1 - first, 1, 1 - to)]
    deals += [deal(kind, 3, to) for kind in (0, 1) for to in (0, 1)]
    for copy in deals:
        copy.start()

    def forward(kind, way, step, p):
        by = 1 if way == 0 else -1
        chunk = along(pos[kind], -by * step)
        block = piece(kind, chunk, p)
        return send(block, block, g_send.at[kind, way, step, SLOT[p]], g_recv.at[kind, chunk, SLOT[p]], neighbour(kind, by))

    def arrived(kind, way, step, p):
        by = 1 if way == 0 else -1
        chunk = along(pos[kind], -by * step)
        block = piece(kind, chunk, p)
        return send(block, block, g_send.at[kind, way, 0, 0], g_recv.at[kind, chunk, SLOT[p]], neighbour(kind, by))

    def quarter(q):
        return pl.ds(q * 128, 128)

    def last(way, q):
        by = 1 if way == 0 else -1
        block = pair(0, along(z, -by * 3), "AB"[way]).at[:, :, :, quarter(q)]
        return send(block, block, l_send.at[way, q], l_recv.at[way, q], neighbour(0, by))

    def last_arrived(way, q):
        block = pair(0, along(z, 4), "AB"[way]).at[:, :, :, quarter(q)]
        return send(block, block, l_send.at[way, q], l_recv.at[way, q], neighbour(0, 1))

    sent = list(deals)
    taken = set()

    def new(*key):
        first = key not in taken
        taken.add(key)
        return first

    def come(kind, way, step, p):
        if new(kind, way, step, p):
            arrived(kind, way, step, p).wait_recv()

    def take(kind, way, step, p):
        for unit in UNITS[p]:
            if step > 0:
                for k, w, s, block in TURNS:
                    if (k, w, s) == (kind, way, step - 1) and unit in UNITS[block]:
                        come(kind, way, step, block)
            elif not new(kind, unit):
                continue
            elif unit == "a":
                own[kind].wait()
            elif unit == "b":
                dealt(kind, 0, other).wait_recv()
            else:
                dealt(kind, unit, 0).wait_recv()
                dealt(kind, unit, 1).wait_recv()

    def go(copies):
        for copy in copies:
            copy.start()
            sent.append(copy)

    for kind, way, step, p in TURNS:
        take(kind, way, step, p)
        if kind == 0 and step == 3:
            go([last(way, q) for q in range(4)])
        else:
            go([forward(kind, way, step, p)])

    def rest(kind, units):
        for k, way, step, p in TURNS:
            if k == kind and (kind, step) != (0, 3) and any(unit in units for unit in UNITS[p]):
                come(kind, way, step + 1, p)

    def product(p, nears, columns):
        x_from, total = step_x(p), None
        for near in nears:
            chunk = along(z, near)
            for part in (0, 1):
                left = yg[chunk, part, x_from // 2, lax.rem(x_from, 2)]
                right = xg[chunk, part, :, :, :, columns]
                right = right.reshape(256, right.shape[-1])
                term = jnp.dot(left, right, preferred_element_type=jnp.float32)
                total = term if total is None else total + term
        return total

    def hand(p, q):
        return send(
            tile.at[p, quarter(q)],
            out_ref.at[x, quarter(q)],
            c_send.at[p, q],
            c_recv.at[BACK[p], q],
            at(row, z, step_x(p), layer),
        )

    def handed(p, q):
        block = out_ref.at[step_x(p), quarter(q)]
        return send(block, block, c_send.at[p, q], c_recv.at[p, q], at(row, z, step_x(p), layer))

    def early(p):
        acc[p] = product(p, (0, 1, -1, 2, -2, 3, -3), slice(None))

    def finish(p, q):
        block = (acc[p, :, quarter(q)] + product(p, (4,), quarter(q))).T.astype(jnp.bfloat16)
        if p == 0:
            out_ref[x, quarter(q)] = block
        else:
            tile[p, quarter(q)] = block
            go([hand(p, q)])

    rest(0, ("a", "b", 1, 2, 3))
    rest(1, (2, 3))
    early(3)
    early(2)
    for q in range(4):
        for way in (0, 1):
            last_arrived(way, q).wait_recv()
        finish(3, q)
        finish(2, q)
        if q == 1:
            rest(1, (1,))
            early(1)
            finish(1, 0)
        if q >= 1:
            finish(1, q)
    rest(1, ("a", "b"))
    early(0)
    for q in range(4):
        finish(0, q)
    for copy in sent:
        copy.wait_send()
    for p in (1, 2, 3):
        for q in range(4):
            handed(p, q).wait_recv()


def on_device(anomaly_x, anomaly_y):
    dma = pltpu.SemaphoreType.DMA
    return pl.pallas_call(
        kernel,
        out_shape=pltpu.VMEM((4, 512, 128), jnp.bfloat16),
        in_specs=[pl.BlockSpec(memory_space=pl.ANY)] * 2,
        out_specs=pl.BlockSpec(memory_space=pltpu.VMEM),
        scratch_shapes=[
            pltpu.VMEM((8, 64, 512), jnp.bfloat16),
            pltpu.VMEM((8, 128, 256), jnp.bfloat16),
            pltpu.VMEM((RING, 2, 2, 2, 64, 512), jnp.bfloat16),
            pltpu.VMEM((RING, 2, 2, 2, 128, 256), jnp.bfloat16),
            pltpu.VMEM((LINE, 128, 512), jnp.float32),
            pltpu.VMEM((LINE, 512, 128), jnp.bfloat16),
            dma((2,)),
            dma((2,)),
            dma((2, LINE, 2)),
            dma((2, LINE, 2)),
            dma((2, 2, 4, 7)),
            dma((2, RING, 7)),
            dma((2, 4)),
            dma((2, 4)),
            dma((LINE, 4)),
            dma((LINE, 4)),
        ],
        compiler_params=pltpu.CompilerParams(collective_id=0, has_side_effects=True),
    )(jnp.transpose(anomaly_x, (0, 2, 1)), anomaly_y)


def solution(mesh):
    placed = (P(None, "row", ("layer", "col")), P(None, "col", ("layer", "row")))
    return jax.shard_map(
        on_device, mesh=mesh, in_specs=placed, out_specs=P("layer", "row", "col"), check_vma=False
    )
```

```python
import jax
import jax.numpy as jnp
from jax import lax
from jax.experimental import pallas as pl
from jax.experimental.pallas import tpu as pltpu
from jax.sharding import PartitionSpec as P

MESH = pl.DeviceIdType.MESH
RING = 8
LINE = 4
OFFSETS = (0, 1, 3, 2)
BACK = (0, 2, 1, 3)
UNITS = {"a": ("a",), "b": ("b",), 0: ("a", "b"), 1: (1,), 2: (2,), 3: (3,), "A": ("a", "b", 3), "B": (1, 2)}
TURNS = (
    (0, 0, 0, "a"), (0, 1, 0, "a"), (1, 0, 0, "a"), (1, 1, 0, "a"), (0, 0, 0, "b"), (0, 1, 0, "b"),
    (1, 0, 0, "b"), (1, 1, 0, "b"), (0, 0, 1, "a"), (0, 1, 1, "a"), (1, 1, 1, "a"), (1, 0, 0, 2),
    (0, 0, 0, 1), (0, 1, 0, 1), (1, 0, 1, "a"), (1, 1, 0, 2), (0, 0, 0, 2), (0, 1, 0, 2),
    (1, 0, 0, 1), (1, 1, 0, 1), (0, 0, 1, "b"), (0, 1, 1, "b"), (1, 1, 1, "b"), (1, 0, 1, "b"),
    (1, 0, 1, 2), (0, 0, 1, 1), (0, 1, 1, 1), (1, 1, 1, 2), (1, 1, 1, 1), (0, 0, 0, 3),
    (0, 1, 0, 3), (0, 0, 1, 2), (0, 1, 1, 2), (1, 0, 0, 3), (1, 0, 1, 1), (1, 1, 0, 3),
    (0, 1, 2, 1), (1, 1, 2, 2), (0, 0, 1, 3), (0, 0, 2, 0), (0, 1, 1, 3), (1, 0, 1, 3),
    (1, 0, 2, 0), (1, 1, 1, 3), (0, 1, 2, 2), (1, 1, 2, 1), (0, 1, 2, 0), (1, 1, 3, 2),
    (0, 0, 2, 3), (0, 0, 2, "B"), (1, 0, 2, 3), (1, 0, 2, 2), (0, 1, 2, 3), (1, 1, 2, 3),
    (0, 1, 3, "B"), (1, 1, 3, 1), (0, 0, 3, "A"), (1, 0, 3, 3), (1, 0, 2, 1), (1, 1, 2, 0),
    (1, 0, 3, 0),)
SLOT = {turn: i for i, turn in enumerate(t for t in TURNS if (t[0], t[2]) != (0, 3))}


def kernel(
    x_hbm, y_hbm, out_ref, x_in, y_in, xg, yg, acc, tile, in_sem, own_sem,
    a_send, a_recv, g_send, g_recv, l_recv, c_send, c_recv,
):
    row, col, layer = lax.axis_index("row"), lax.axis_index("col"), lax.axis_index("layer")
    z, x = col // LINE, lax.rem(col, LINE)
    other = 1 - layer
    mine = layer * LINE + x

    def at(row_to, z_to, x_to, layer_to):
        return {"row": row_to, "col": z_to * LINE + x_to, "layer": layer_to}

    def step_x(p):
        return lax.rem(x + OFFSETS[p], LINE)

    def along(pos, by):
        return lax.rem(pos + by + RING, RING)

    def send(src, dst, send_sem, recv_sem, device_id):
        return pltpu.make_async_remote_copy(
            src_ref=src, dst_ref=dst, send_sem=send_sem, recv_sem=recv_sem, device_id=device_id, device_id_type=MESH
        )

    pos = (z, row)
    inputs = (x_in, y_in)
    gathered = (xg, yg)

    def place(kind, chunk, part, x_from):
        return gathered[kind].at[chunk, part, x_from // 2, lax.rem(x_from, 2)]

    def pair(kind, chunk, which):
        parity = lax.rem(x + (0 if which == "A" else 1), 2)
        return gathered[kind].at[chunk, :, :, parity]

    def piece(kind, chunk, p):
        if p in ("A", "B"):
            return pair(kind, chunk, p)
        if p in ("a", "b"):
            return place(kind, chunk, layer if p == "a" else other, x)
        return place(kind, chunk, slice(None), step_x(p))

    def neighbour(kind, by):
        return at(row, along(z, by), x, layer) if kind == 0 else at(along(row, by), z, x, layer)

    loads = [
        pltpu.make_async_copy(x_hbm, x_in, in_sem.at[0]),
        pltpu.make_async_copy(y_hbm, y_in, in_sem.at[1]),
    ]
    own = [
        pltpu.make_async_copy(x_hbm.at[mine], place(0, z, layer, x), own_sem.at[0]),
        pltpu.make_async_copy(y_hbm.at[mine], place(1, row, layer, x), own_sem.at[1]),
    ]
    for copy in loads + own:
        copy.start()

    barrier = pltpu.get_barrier_semaphore()
    peers = [at(row, z, x, other)]
    peers += [at(row, z, step_x(p), to) for p in (1, 2, 3) for to in (0, 1)]
    peers += [neighbour(kind, by) for kind in (0, 1) for by in (1, -1)]
    for peer in peers:
        pl.semaphore_signal(barrier, inc=1, device_id=peer, device_id_type=MESH)
    pl.semaphore_wait(barrier, len(peers))
    for copy in loads:
        copy.wait()

    def deal(kind, p, to):
        x_to = step_x(p)
        return send(
            inputs[kind].at[to * LINE + x_to],
            place(kind, pos[kind], layer, x),
            a_send.at[kind],
            a_recv.at[kind, BACK[p]],
            at(row, z, x_to, to),
        )

    def dealt(kind, p):
        part = other if p == 0 else slice(None)
        block = place(kind, pos[kind], part, step_x(p))
        return send(block, block, a_send.at[kind], a_recv.at[kind, p], at(row, z, x, other))

    deals = [deal(kind, 0, other) for kind in (0, 1)]
    for first, to in ((0, 0), (0, 1), (1, 0), (1, 1)):
        deals += [deal(first, 2, to), deal(1 - first, 1, 1 - to)]
    deals += [deal(kind, 3, to) for kind in (0, 1) for to in (0, 1)]
    for copy in deals:
        copy.start()

    def forward(kind, way, step, p):
        by = 1 if way == 0 else -1
        chunk = along(pos[kind], -by * step)
        block = piece(kind, chunk, p)
        return send(block, block, g_send.at[kind], g_recv.at[SLOT[kind, way, step, p]], neighbour(kind, by))

    def arrived(kind, way, step, p):
        by = 1 if way == 0 else -1
        chunk = along(pos[kind], -by * step)
        block = piece(kind, chunk, p)
        return send(block, block, g_send.at[kind], g_recv.at[SLOT[kind, way, step - 1, p]], neighbour(kind, by))

    def quarter(q):
        return pl.ds(q * 128, 128)

    def last(way, q):
        by = 1 if way == 0 else -1
        block = pair(0, along(z, -by * 3), "AB"[way]).at[:, :, :, quarter(q)]
        return send(block, block, g_send.at[0], l_recv.at[q], neighbour(0, by))

    def last_arrived(q):
        block = xg.at[along(z, 4), :, :, :, :, quarter(q)]
        return send(block, block, g_send.at[0], l_recv.at[q], neighbour(0, 1))

    taken = set()

    def new(*key):
        first = key not in taken
        taken.add(key)
        return first

    def come(kind, way, step, p):
        if new(kind, way, step, p):
            arrived(kind, way, step, p).wait_recv()

    def take(kind, way, step, p):
        for unit in UNITS[p]:
            if step > 0:
                for k, w, s, block in TURNS:
                    if (k, w, s) == (kind, way, step - 1) and unit in UNITS[block]:
                        come(kind, way, step, block)
            elif not new(kind, unit):
                continue
            elif unit == "a":
                own[kind].wait()
            elif unit == "b":
                dealt(kind, 0).wait_recv()
            else:
                dealt(kind, unit).wait_recv()

    def go(copies):
        for copy in copies:
            copy.start()

    for kind, way, step, p in TURNS:
        take(kind, way, step, p)
        if kind == 0 and step == 3:
            go([last(way, q) for q in range(4)])
        else:
            go([forward(kind, way, step, p)])

    def rest(kind, units):
        for k, way, step, p in TURNS:
            if k == kind and (kind, step) != (0, 3) and any(unit in units for unit in UNITS[p]):
                come(kind, way, step + 1, p)

    def product(p, nears, columns):
        x_from, total = step_x(p), None
        for near in nears:
            chunk = along(z, near)
            for part in (0, 1):
                left = yg[chunk, part, x_from // 2, lax.rem(x_from, 2)]
                right = xg[chunk, part, :, :, :, columns]
                right = right.reshape(256, right.shape[-1])
                term = jnp.dot(left, right, preferred_element_type=jnp.float32)
                total = term if total is None else total + term
        return total

    def hand(p, q):
        return send(
            tile.at[p, quarter(q)],
            out_ref.at[x, quarter(q)],
            c_send,
            c_recv,
            at(row, z, step_x(p), layer),
        )

    def early(p):
        acc[p] = product(p, (0, 1, -1, 2, -2, 3, -3), slice(None))

    def finish(p, q):
        block = (acc[p, :, quarter(q)] + product(p, (4,), quarter(q))).T.astype(jnp.bfloat16)
        if p == 0:
            out_ref[x, quarter(q)] = block
        else:
            tile[p, quarter(q)] = block
            go([hand(p, q)])

    rest(0, ("a", "b", 1, 2, 3))
    rest(1, (2, 3))
    early(3)
    early(2)
    for q in range(4):
        last_arrived(q).wait_recv()
        finish(3, q)
        finish(2, q)
        if q == 1:
            rest(1, (1,))
            early(1)
            finish(1, 0)
        if q >= 1:
            finish(1, q)
    rest(1, ("a", "b"))
    early(0)
    for q in range(4):
        finish(0, q)
    for kind in (0, 1):
        batches, chunks = inputs[kind].at[: RING - 1], gathered[kind].at[: RING - 1]
        send(batches, batches, a_send.at[kind], a_recv.at[kind, 0], neighbour(kind, 1)).wait_send()
        send(chunks, chunks, g_send.at[kind], g_recv.at[0], neighbour(kind, 1)).wait_send()
    tiles = tile.at[1:]
    handed = send(tiles, tiles, c_send, c_recv, at(row, z, step_x(1), layer))
    handed.wait_send()
    handed.wait_recv()


def on_device(anomaly_x, anomaly_y):
    dma = pltpu.SemaphoreType.DMA
    return pl.pallas_call(
        kernel,
        out_shape=pltpu.VMEM((4, 512, 128), jnp.bfloat16),
        in_specs=[pl.BlockSpec(memory_space=pl.ANY)] * 2,
        out_specs=pl.BlockSpec(memory_space=pltpu.VMEM),
        scratch_shapes=[
            pltpu.VMEM((8, 64, 512), jnp.bfloat16),
            pltpu.VMEM((8, 128, 256), jnp.bfloat16),
            pltpu.VMEM((RING, 2, 2, 2, 64, 512), jnp.bfloat16),
            pltpu.VMEM((RING, 2, 2, 2, 128, 256), jnp.bfloat16),
            pltpu.VMEM((LINE, 128, 512), jnp.float32),
            pltpu.VMEM((LINE, 512, 128), jnp.bfloat16),
            dma((2,)),
            dma((2,)),
            dma((2,)),
            dma((2, LINE)),
            dma((2,)),
            dma((len(SLOT),)),
            dma((4,)),
            dma,
            dma,
        ],
        compiler_params=pltpu.CompilerParams(collective_id=0, has_side_effects=True),
    )(jnp.transpose(anomaly_x, (0, 2, 1)), anomaly_y)


def solution(mesh):
    placed = (P(None, "row", ("layer", "col")), P(None, "col", ("layer", "row")))
    return jax.shard_map(
        on_device, mesh=mesh, in_specs=placed, out_specs=P("layer", "row", "col"), check_vma=False
    )
```

```python
import jax
import jax.numpy as jnp
from jax import lax
from jax.experimental import pallas as pl
from jax.experimental.pallas import tpu as pltpu
from jax.sharding import PartitionSpec as P

MESH = pl.DeviceIdType.MESH
RING = 8
LINE = 4
OFFSETS = (0, 1, 3, 2)
BACK = (0, 2, 1, 3)
UNITS = {"a": ("a",), "b": ("b",), 0: ("a", "b"), 1: (1,), 2: (2,), 3: (3,), "A": ("a", "b", 3), "B": (1, 2)}
TURNS = (
    (0, 0, 0, "a"), (0, 1, 0, "a"), (1, 0, 0, "a"), (1, 1, 0, "a"), (0, 0, 0, "b"), (0, 1, 0, "b"),
    (1, 0, 0, "b"), (1, 1, 0, "b"), (0, 0, 1, "a"), (0, 1, 1, "a"), (1, 1, 1, "a"), (1, 0, 0, 2),
    (0, 0, 0, 1), (0, 1, 0, 1), (1, 0, 1, "a"), (1, 1, 0, 2), (0, 0, 0, 2), (0, 1, 0, 2),
    (1, 0, 0, 1), (1, 1, 0, 1), (0, 0, 1, "b"), (0, 1, 1, "b"), (1, 1, 1, "b"), (1, 0, 1, "b"),
    (1, 0, 1, 2), (0, 0, 1, 1), (0, 1, 1, 1), (1, 1, 1, 2), (1, 1, 1, 1), (0, 0, 0, 3),
    (0, 1, 0, 3), (0, 0, 1, 2), (0, 1, 1, 2), (1, 0, 0, 3), (1, 0, 1, 1), (1, 1, 0, 3),
    (0, 1, 2, 1), (1, 1, 2, 2), (0, 0, 1, 3), (0, 0, 2, 0), (0, 1, 1, 3), (1, 0, 1, 3),
    (1, 0, 2, 0), (1, 1, 1, 3), (0, 1, 2, 2), (1, 1, 2, 1), (0, 1, 2, 0), (1, 1, 3, 2),
    (0, 0, 2, 3), (0, 0, 2, "B"), (1, 0, 2, 3), (1, 0, 2, 2), (0, 1, 2, 3), (1, 1, 2, 3),
    (0, 1, 3, "B"), (1, 1, 3, 1), (0, 0, 3, "A"), (1, 0, 3, 3), (1, 0, 2, 1), (1, 1, 2, 0),
    (1, 0, 3, 0),)
SLOT = {turn: i for i, turn in enumerate(t for t in TURNS if (t[0], t[2]) != (0, 3))}


def kernel(
    x_hbm, y_hbm, out_ref, x_in, y_in, xg, yg, acc, tile, in_sem, own_sem,
    a_send, a_recv, g_send, g_recv, l_recv, c_send, c_recv,
):
    row, col, layer = lax.axis_index("row"), lax.axis_index("col"), lax.axis_index("layer")
    z, x = col // LINE, lax.rem(col, LINE)
    other = 1 - layer
    mine = layer * LINE + x

    def at(row_to, z_to, x_to, layer_to):
        return {"row": row_to, "col": z_to * LINE + x_to, "layer": layer_to}

    def step_x(p):
        return lax.rem(x + OFFSETS[p], LINE)

    def along(pos, by):
        return lax.rem(pos + by + RING, RING)

    def send(src, dst, send_sem, recv_sem, device_id):
        return pltpu.make_async_remote_copy(
            src_ref=src, dst_ref=dst, send_sem=send_sem, recv_sem=recv_sem, device_id=device_id, device_id_type=MESH
        )

    pos = (z, row)
    inputs = (x_in, y_in)
    gathered = (xg, yg)

    def place(kind, chunk, part, x_from):
        return gathered[kind].at[chunk, part, x_from // 2, lax.rem(x_from, 2)]

    def pair(kind, chunk, which):
        parity = lax.rem(x + (0 if which == "A" else 1), 2)
        return gathered[kind].at[chunk, :, :, parity]

    def piece(kind, chunk, p):
        if p in ("A", "B"):
            return pair(kind, chunk, p)
        if p in ("a", "b"):
            return place(kind, chunk, layer if p == "a" else other, x)
        return place(kind, chunk, slice(None), step_x(p))

    def neighbour(kind, by):
        return at(row, along(z, by), x, layer) if kind == 0 else at(along(row, by), z, x, layer)

    loads = [
        pltpu.make_async_copy(x_hbm, x_in, in_sem.at[0]),
        pltpu.make_async_copy(y_hbm, y_in, in_sem.at[1]),
    ]
    own = [
        pltpu.make_async_copy(x_hbm.at[mine], place(0, z, layer, x), own_sem.at[0]),
        pltpu.make_async_copy(y_hbm.at[mine], place(1, row, layer, x), own_sem.at[1]),
    ]
    for copy in loads + own:
        copy.start()

    barrier = pltpu.get_barrier_semaphore()
    peers = [at(row, z, x, other)]
    peers += [at(row, z, step_x(p), to) for p in (1, 2, 3) for to in (0, 1)]
    peers += [neighbour(kind, by) for kind in (0, 1) for by in (1, -1)]
    for peer in peers:
        pl.semaphore_signal(barrier, inc=1, device_id=peer, device_id_type=MESH)
    pl.semaphore_wait(barrier, len(peers))
    for copy in loads:
        copy.wait()

    def deal(kind, p, to):
        x_to = step_x(p)
        return send(
            inputs[kind].at[to * LINE + x_to],
            place(kind, pos[kind], layer, x),
            a_send.at[kind],
            a_recv.at[kind, BACK[p]],
            at(row, z, x_to, to),
        )

    def dealt(kind, p):
        part = other if p == 0 else slice(None)
        block = place(kind, pos[kind], part, step_x(p))
        return send(block, block, a_send.at[kind], a_recv.at[kind, p], at(row, z, x, other))

    deals = [deal(kind, 0, other) for kind in (0, 1)]
    for first, to in ((0, 0), (0, 1), (1, 0), (1, 1)):
        deals += [deal(first, 2, to), deal(1 - first, 1, 1 - to)]
    deals += [deal(kind, 3, to) for kind in (0, 1) for to in (0, 1)]
    for copy in deals:
        copy.start()

    def forward(kind, way, step, p):
        by = 1 if way == 0 else -1
        chunk = along(pos[kind], -by * step)
        block = piece(kind, chunk, p)
        return send(block, block, g_send.at[kind], g_recv.at[SLOT[kind, way, step, p]], neighbour(kind, by))

    def arrived(kind, way, step, p):
        by = 1 if way == 0 else -1
        chunk = along(pos[kind], -by * step)
        block = piece(kind, chunk, p)
        return send(block, block, g_send.at[kind], g_recv.at[SLOT[kind, way, step - 1, p]], neighbour(kind, by))

    def quarter(q):
        return pl.ds(q * 128, 128)

    def last(way, q):
        by = 1 if way == 0 else -1
        block = pair(0, along(z, -by * 3), "AB"[way]).at[:, :, :, quarter(q)]
        return send(block, block, g_send.at[0], l_recv.at[q], neighbour(0, by))

    def last_arrived(q):
        block = xg.at[along(z, 4), :, :, :, :, quarter(q)]
        return send(block, block, g_send.at[0], l_recv.at[q], neighbour(0, 1))

    taken = set()

    def new(*key):
        first = key not in taken
        taken.add(key)
        return first

    def come(kind, way, step, p):
        if new(kind, way, step, p):
            arrived(kind, way, step, p).wait_recv()

    def take(kind, way, step, p):
        for unit in UNITS[p]:
            if step > 0:
                for k, w, s, block in TURNS:
                    if (k, w, s) == (kind, way, step - 1) and unit in UNITS[block]:
                        come(kind, way, step, block)
            elif not new(kind, unit):
                continue
            elif unit == "a":
                own[kind].wait()
            elif unit == "b":
                dealt(kind, 0).wait_recv()
            else:
                dealt(kind, unit).wait_recv()

    def go(copies):
        for copy in copies:
            copy.start()

    for kind, way, step, p in TURNS:
        take(kind, way, step, p)
        if kind == 0 and step == 3:
            go([last(way, q) for q in range(4)])
        else:
            go([forward(kind, way, step, p)])

    def rest(kind, units):
        for k, way, step, p in TURNS:
            if k == kind and (kind, step) != (0, 3) and any(unit in units for unit in UNITS[p]):
                come(kind, way, step + 1, p)

    def product(p, nears, columns):
        x_from, total = step_x(p), None
        for near in nears:
            chunk = along(z, near)
            for part in (0, 1):
                left = yg[chunk, part, x_from // 2, lax.rem(x_from, 2)]
                right = xg[chunk, part, :, :, :, columns]
                right = right.reshape(256, right.shape[-1])
                term = jnp.dot(left, right, preferred_element_type=jnp.float32)
                total = term if total is None else total + term
        return total

    def hand(p, q):
        return send(
            tile.at[p, quarter(q)],
            out_ref.at[x, quarter(q)],
            c_send,
            c_recv,
            at(row, z, step_x(p), layer),
        )

    def early(p):
        acc[p] = product(p, (0, 1, -1, 2, -2, 3, -3), slice(None))

    def finish(p, q):
        block = (acc[p, :, quarter(q)] + product(p, (4,), quarter(q))).T.astype(jnp.bfloat16)
        if p == 0:
            out_ref[x, quarter(q)] = block
        else:
            tile[p, quarter(q)] = block
            go([hand(p, q)])

    rest(0, ("a", "b", 1, 2, 3))
    rest(1, (2, 3))
    early(3)
    early(2)
    for q in range(4):
        last_arrived(q).wait_recv()
        finish(3, q)
        finish(2, q)
        if q == 0:
            rest(1, (1,))
            early(1)
        finish(1, q)
    rest(1, ("a", "b"))
    early(0)
    for q in range(4):
        finish(0, q)
    for kind in (0, 1):
        batches, chunks = inputs[kind].at[: RING - 1], gathered[kind].at[: RING - 1]
        send(batches, batches, a_send.at[kind], a_recv.at[kind, 0], neighbour(kind, 1)).wait_send()
        send(chunks, chunks, g_send.at[kind], g_recv.at[0], neighbour(kind, 1)).wait_send()
    tiles = tile.at[1:]
    handed = send(tiles, tiles, c_send, c_recv, at(row, z, step_x(1), layer))
    handed.wait_send()
    handed.wait_recv()


def on_device(anomaly_x, anomaly_y):
    dma = pltpu.SemaphoreType.DMA
    return pl.pallas_call(
        kernel,
        out_shape=pltpu.VMEM((4, 512, 128), jnp.bfloat16),
        in_specs=[pl.BlockSpec(memory_space=pl.ANY)] * 2,
        out_specs=pl.BlockSpec(memory_space=pltpu.VMEM),
        scratch_shapes=[
            pltpu.VMEM((8, 64, 512), jnp.bfloat16),
            pltpu.VMEM((8, 128, 256), jnp.bfloat16),
            pltpu.VMEM((RING, 2, 2, 2, 64, 512), jnp.bfloat16),
            pltpu.VMEM((RING, 2, 2, 2, 128, 256), jnp.bfloat16),
            pltpu.VMEM((LINE, 128, 512), jnp.float32),
            pltpu.VMEM((LINE, 512, 128), jnp.bfloat16),
            dma((2,)),
            dma((2,)),
            dma((2,)),
            dma((2, LINE)),
            dma((2,)),
            dma((len(SLOT),)),
            dma((4,)),
            dma,
            dma,
        ],
        compiler_params=pltpu.CompilerParams(collective_id=0, has_side_effects=True),
    )(jnp.transpose(anomaly_x, (0, 2, 1)), anomaly_y)


def solution(mesh):
    placed = (P(None, "row", ("layer", "col")), P(None, "col", ("layer", "row")))
    return jax.shard_map(
        on_device, mesh=mesh, in_specs=placed, out_specs=P("layer", "row", "col"), check_vma=False
    )
```

```python
import jax
import jax.numpy as jnp
from jax import lax
from jax.experimental import pallas as pl
from jax.experimental.pallas import tpu as pltpu
from jax.sharding import PartitionSpec as P

MESH = pl.DeviceIdType.MESH
RING = 8
LINE = 4
OFFSETS = (0, 1, 3, 2)
BACK = (0, 2, 1, 3)
UNITS = {"a": ("a",), "b": ("b",), 0: ("a", "b"), 1: (1,), 2: (2,), 3: (3,), "A": ("a", "b", 3), "B": (1, 2)}
TURNS = (
    (0, 0, 0, "a"), (0, 1, 0, "a"), (1, 0, 0, "a"), (1, 1, 0, "a"), (0, 0, 0, "b"), (0, 1, 0, "b"),
    (1, 0, 0, "b"), (1, 1, 0, "b"), (0, 0, 1, "a"), (0, 1, 1, "a"), (1, 1, 1, "a"), (1, 0, 0, 2),
    (0, 0, 0, 1), (0, 1, 0, 1), (1, 0, 1, "a"), (1, 1, 0, 2), (0, 0, 0, 2), (0, 1, 0, 2),
    (1, 0, 0, 1), (1, 1, 0, 1), (0, 0, 1, "b"), (0, 1, 1, "b"), (1, 1, 1, "b"), (1, 0, 1, "b"),
    (1, 0, 1, 2), (0, 0, 1, 1), (0, 1, 1, 1), (1, 1, 1, 2), (1, 1, 1, 1), (0, 0, 0, 3),
    (0, 1, 0, 3), (0, 0, 1, 2), (0, 1, 1, 2), (1, 0, 0, 3), (1, 0, 1, 1), (1, 1, 0, 3),
    (0, 1, 2, 1), (1, 1, 2, 2), (0, 0, 1, 3), (0, 0, 2, 0), (0, 1, 1, 3), (1, 0, 1, 3),
    (1, 0, 2, 0), (1, 1, 1, 3), (0, 1, 2, 2), (1, 1, 2, 1), (0, 1, 2, 0), (1, 1, 3, 2),
    (0, 0, 2, 3), (0, 0, 2, "B"), (1, 0, 2, 3), (1, 0, 2, 2), (0, 1, 2, 3), (1, 1, 2, 3),
    (0, 1, 3, "B"), (1, 1, 3, 1), (0, 0, 3, "A"), (1, 0, 3, 3), (1, 0, 2, 1), (1, 1, 2, 0),
    (1, 0, 3, 0),)
SLOT = {turn: i for i, turn in enumerate(t for t in TURNS if (t[0], t[2]) != (0, 3))}


def kernel(
    x_hbm, y_hbm, out_ref, x_in, y_in, xg, yg, acc, tile, in_sem, own_sem,
    a_send, a_recv, g_send, g_recv, l_recv, c_send, c_recv,
):
    row, col, layer = lax.axis_index("row"), lax.axis_index("col"), lax.axis_index("layer")
    z, x = col // LINE, lax.rem(col, LINE)
    other = 1 - layer
    mine = layer * LINE + x

    def at(row_to, z_to, x_to, layer_to):
        return {"row": row_to, "col": z_to * LINE + x_to, "layer": layer_to}

    def step_x(p):
        return lax.rem(x + OFFSETS[p], LINE)

    def along(pos, by):
        return lax.rem(pos + by + RING, RING)

    def send(src, dst, send_sem, recv_sem, device_id):
        return pltpu.make_async_remote_copy(
            src_ref=src, dst_ref=dst, send_sem=send_sem, recv_sem=recv_sem, device_id=device_id, device_id_type=MESH
        )

    pos = (z, row)
    inputs = (x_in, y_in)
    gathered = (xg, yg)

    def place(kind, chunk, part, x_from):
        return gathered[kind].at[chunk, part, x_from // 2, lax.rem(x_from, 2)]

    def pair(kind, chunk, which):
        parity = lax.rem(x + (0 if which == "A" else 1), 2)
        return gathered[kind].at[chunk, :, :, parity]

    def piece(kind, chunk, p):
        if p in ("A", "B"):
            return pair(kind, chunk, p)
        if p in ("a", "b"):
            return place(kind, chunk, layer if p == "a" else other, x)
        return place(kind, chunk, slice(None), step_x(p))

    def neighbour(kind, by):
        return at(row, along(z, by), x, layer) if kind == 0 else at(along(row, by), z, x, layer)

    loads = [
        pltpu.make_async_copy(x_hbm, x_in, in_sem.at[0]),
        pltpu.make_async_copy(y_hbm, y_in, in_sem.at[1]),
    ]
    own = [
        pltpu.make_async_copy(x_hbm.at[mine], place(0, z, layer, x), own_sem.at[0]),
        pltpu.make_async_copy(y_hbm.at[mine], place(1, row, layer, x), own_sem.at[1]),
    ]
    for copy in loads + own:
        copy.start()

    barrier = pltpu.get_barrier_semaphore()
    peers = [at(row, z, x, other)]
    peers += [at(row, z, step_x(p), to) for p in (1, 2, 3) for to in (0, 1)]
    peers += [neighbour(kind, by) for kind in (0, 1) for by in (1, -1)]
    for peer in peers:
        pl.semaphore_signal(barrier, inc=1, device_id=peer, device_id_type=MESH)
    pl.semaphore_wait(barrier, len(peers))
    for copy in loads:
        copy.wait()

    def deal(kind, p, to):
        x_to = step_x(p)
        return send(
            inputs[kind].at[to * LINE + x_to],
            place(kind, pos[kind], layer, x),
            a_send.at[kind],
            a_recv.at[kind, BACK[p]],
            at(row, z, x_to, to),
        )

    def dealt(kind, p):
        part = other if p == 0 else slice(None)
        block = place(kind, pos[kind], part, step_x(p))
        return send(block, block, a_send.at[kind], a_recv.at[kind, p], at(row, z, x, other))

    deals = [deal(kind, 0, other) for kind in (0, 1)]
    for first, to in ((0, 0), (0, 1), (1, 0), (1, 1)):
        deals += [deal(first, 2, to), deal(1 - first, 1, 1 - to)]
    deals += [deal(kind, 3, to) for kind in (0, 1) for to in (0, 1)]
    for copy in deals:
        copy.start()

    def forward(kind, way, step, p):
        by = 1 if way == 0 else -1
        chunk = along(pos[kind], -by * step)
        block = piece(kind, chunk, p)
        return send(block, block, g_send.at[kind], g_recv.at[SLOT[kind, way, step, p]], neighbour(kind, by))

    def arrived(kind, way, step, p):
        by = 1 if way == 0 else -1
        chunk = along(pos[kind], -by * step)
        block = piece(kind, chunk, p)
        return send(block, block, g_send.at[kind], g_recv.at[SLOT[kind, way, step - 1, p]], neighbour(kind, by))

    def quarter(q):
        return pl.ds(q * 128, 128)

    def last(way, q):
        by = 1 if way == 0 else -1
        block = pair(0, along(z, -by * 3), "AB"[way]).at[:, :, :, quarter(q)]
        return send(block, block, g_send.at[0], l_recv.at[q], neighbour(0, by))

    def last_arrived(q):
        block = xg.at[along(z, 4), :, :, :, :, quarter(q)]
        return send(block, block, g_send.at[0], l_recv.at[q], neighbour(0, 1))

    taken = set()

    def new(*key):
        first = key not in taken
        taken.add(key)
        return first

    def come(kind, way, step, p):
        if new(kind, way, step, p):
            arrived(kind, way, step, p).wait_recv()

    def take(kind, way, step, p):
        for unit in UNITS[p]:
            if step > 0:
                for k, w, s, block in TURNS:
                    if (k, w, s) == (kind, way, step - 1) and unit in UNITS[block]:
                        come(kind, way, step, block)
            elif not new(kind, unit):
                continue
            elif unit == "a":
                own[kind].wait()
            elif unit == "b":
                dealt(kind, 0).wait_recv()
            else:
                dealt(kind, unit).wait_recv()

    def go(copies):
        for copy in copies:
            copy.start()

    for kind, way, step, p in TURNS:
        take(kind, way, step, p)
        if kind == 0 and step == 3:
            go([last(way, q) for q in range(4)])
        else:
            go([forward(kind, way, step, p)])

    def rest(kind, units):
        for k, way, step, p in TURNS:
            if k == kind and (kind, step) != (0, 3) and any(unit in units for unit in UNITS[p]):
                come(kind, way, step + 1, p)

    def product(p, nears, columns):
        x_from, total = step_x(p), None
        for near in nears:
            chunk = along(z, near)
            for part in (0, 1):
                left = yg[chunk, part, x_from // 2, lax.rem(x_from, 2)]
                right = xg[chunk, part, :, :, :, columns]
                right = right.reshape(256, right.shape[-1])
                term = jnp.dot(left, right, preferred_element_type=jnp.float32)
                total = term if total is None else total + term
        return total

    def hand(p, q):
        rows = pl.ds(0, 256) if (p, q) == (1, 1) else quarter(q)
        return send(
            tile.at[p, rows],
            out_ref.at[x, rows],
            c_send,
            c_recv,
            at(row, z, step_x(p), layer),
        )

    def early(p):
        acc[p] = product(p, (0, 1, -1, 2, -2, 3, -3), slice(None))

    def finish(p, q):
        block = (acc[p, :, quarter(q)] + product(p, (4,), quarter(q))).T.astype(jnp.bfloat16)
        if p == 0:
            out_ref[x, quarter(q)] = block
        else:
            tile[p, quarter(q)] = block
            if (p, q) != (1, 0):
                go([hand(p, q)])

    rest(0, ("a", "b", 1, 2, 3))
    rest(1, (2, 3))
    early(3)
    early(2)
    for q in range(4):
        last_arrived(q).wait_recv()
        finish(3, q)
        finish(2, q)
        if q == 0:
            rest(1, (1,))
            early(1)
        finish(1, q)
    rest(1, ("a", "b"))
    early(0)
    for q in range(4):
        finish(0, q)
    for kind in (0, 1):
        batches, chunks = inputs[kind].at[: RING - 1], gathered[kind].at[: RING - 1]
        send(batches, batches, a_send.at[kind], a_recv.at[kind, 0], neighbour(kind, 1)).wait_send()
        send(chunks, chunks, g_send.at[kind], g_recv.at[0], neighbour(kind, 1)).wait_send()
    tiles = tile.at[1:]
    handed = send(tiles, tiles, c_send, c_recv, at(row, z, step_x(1), layer))
    handed.wait_send()
    handed.wait_recv()


def on_device(anomaly_x, anomaly_y):
    dma = pltpu.SemaphoreType.DMA
    return pl.pallas_call(
        kernel,
        out_shape=pltpu.VMEM((4, 512, 128), jnp.bfloat16),
        in_specs=[pl.BlockSpec(memory_space=pl.ANY)] * 2,
        out_specs=pl.BlockSpec(memory_space=pltpu.VMEM),
        scratch_shapes=[
            pltpu.VMEM((8, 64, 512), jnp.bfloat16),
            pltpu.VMEM((8, 128, 256), jnp.bfloat16),
            pltpu.VMEM((RING, 2, 2, 2, 64, 512), jnp.bfloat16),
            pltpu.VMEM((RING, 2, 2, 2, 128, 256), jnp.bfloat16),
            pltpu.VMEM((LINE, 128, 512), jnp.float32),
            pltpu.VMEM((LINE, 512, 128), jnp.bfloat16),
            dma((2,)),
            dma((2,)),
            dma((2,)),
            dma((2, LINE)),
            dma((2,)),
            dma((len(SLOT),)),
            dma((4,)),
            dma,
            dma,
        ],
        compiler_params=pltpu.CompilerParams(collective_id=0, has_side_effects=True),
    )(jnp.transpose(anomaly_x, (0, 2, 1)), anomaly_y)


def solution(mesh):
    placed = (P(None, "row", ("layer", "col")), P(None, "col", ("layer", "row")))
    return jax.shard_map(
        on_device, mesh=mesh, in_specs=placed, out_specs=P("layer", "row", "col"), check_vma=False
    )
```
